32 devices in a mesh: slab: 16 (over z, y, x), energy: 2 (over core).
Axes of the slice: x: 2, y: 2, z: 4, core: 2. Of those that a mesh axis runs over, the one named last changes fastest.
Arguments:
- onsite_energy: float32 [32, 128], P('slab'), may hold values from -0.3 to 0.3
- onsite_mixing: float32 [32, 128, 128], P('slab'), may hold values from -0.15625 to 0.15625
- hop_strength: float32 [32, 128], P('slab'), may hold values from 0.8 to 1.2
- hop_mixing: float32 [32, 128, 128], P('slab'), may hold values from -0.15625 to 0.15625
- energy: float32 [2], P('energy'), parts along dimension 0, may hold values from -0.4 to 0.4
- broadening: float32 [2], P('energy'), parts along dimension 0, may hold values from 0.01 to 0.025
Outputs:
- green_real: float32 [64, 128, 128], P(('energy', 'slab')), parts along dimension 0
- green_imag: float32 [64, 128, 128], P(('energy', 'slab')), parts along dimension 0
The draws below stay inside these ranges and needn't reach their ends.
There are 2 independent parts, one for each index of `energy`. The reference program is written for one: setup_inputs(seed, part) draws one part's arguments, and reference() takes and returns one part's arrays. A program takes and returns all parts, laid end to end along the dimension named above; an argument that names none is the same for every part. Nothing has to cross between parts.
All inputs are finite; a program needn't handle non-finite values.
Results may differ from the reference program's by a relative error of at most 0.0007.
Values sent between devices are 32-bit elements; how exact they have to be, the bound alone decides.
A program may use at most 128 MiB of HBM per device.

```python
import math
import jax
import jax.numpy as jnp
from jax import lax

ORB = 128
SLABS = 32


def steps_of(own_key, extent, cuts, smallest, largest):
    loudness = 1.0
    for position, shards_of in cuts:
        heights = jax.random.uniform(jax.random.fold_in(jax.random.fold_in(own_key, 6), position), (shards_of,), jnp.float32, smallest / len(cuts), largest / len(cuts))
        loudness = loudness * jnp.repeat(jnp.exp(heights), extent[position] // shards_of).reshape((-1,) + (1,) * (len(extent) - 1 - position))
    return loudness


def centred(rng, shape, scale, bound, pieces=(), kind=jnp.bfloat16):
    drawn = jax.random.normal(rng, shape, jnp.float32) * scale
    if len(pieces) > 0:
        drawn = steps_of(rng, shape, pieces, -0.22, 0.18) * drawn
    return jnp.clip(drawn, min=-bound, max=bound).astype(kind)


def setup_inputs(seed: int = 0, part: int = 0) -> dict:
    seeds = jax.random.split(jax.random.key(seed), 7)
    own_keys = jax.random.split(jax.random.fold_in(seeds[6], part), 7)
    onsite_energy = jnp.clip(jax.random.uniform(seeds[0], (SLABS, ORB), jnp.float32, -0.3, 0.3) * steps_of(seeds[0], (SLABS, ORB), ((0, 16),), -0.4, 0.0), -0.3, 0.3)
    onsite_mixing = centred(seeds[1], (SLABS, ORB, ORB), (10 * ORB) ** -0.5, 0.15625, ((0, 16),), jnp.float32)
    hop_strength = jnp.clip(0.8 + 0.40000004 * jax.random.uniform(seeds[2], (SLABS, ORB), jnp.float32) ** steps_of(seeds[2], (SLABS, ORB), ((0, 16),), -0.2, 0.2), 0.8, 1.2)
    hop_mixing = centred(seeds[3], (SLABS, ORB, ORB), (10 * ORB) ** -0.5, 0.15625, ((0, 16),), jnp.float32)
    energy = jnp.clip(jax.random.uniform(own_keys[4], (1,), jnp.float32, -0.4, 0.4), -0.4, 0.4)
    broadening = jnp.clip(jnp.exp(jax.random.uniform(own_keys[5], (1,), jnp.float32, math.log(0.01), math.log(0.025))), 0.01, 0.025)
    return dict(onsite_energy=onsite_energy, onsite_mixing=onsite_mixing, hop_strength=hop_strength, hop_mixing=hop_mixing, energy=energy, broadening=broadening)


def real_product(first, second):
    return jnp.dot(first.astype(jnp.float32), second.astype(jnp.float32), precision=lax.Precision.HIGHEST, preferred_element_type=jnp.float32)

def complex_product(first, second):
    return (real_product(first[0], second[0]) - real_product(first[1], second[1]), real_product(first[0], second[1]) + real_product(first[1], second[0]))

def invert_exact(real_part, imag_part):
    orbitals = real_part.shape[0]
    stacked = jnp.concatenate([jnp.concatenate([real_part, -imag_part], axis=1), jnp.concatenate([imag_part, real_part], axis=1)], axis=0)
    whole = jnp.linalg.inv(stacked)
    return (whole[:orbitals, :orbitals], whole[orbitals:, :orbitals])

def reference(onsite_energy, onsite_mixing, hop_strength, hop_mixing, energy, broadening):
    orbitals = onsite_mixing.shape[1]
    identity = jnp.eye(orbitals, dtype=jnp.float32)
    hamilton = jax.vmap(jnp.diag)(onsite_energy) + 0.5 * (onsite_mixing + jnp.swapaxes(onsite_mixing, 1, 2))
    diagonal_real = energy[0] * identity - hamilton
    diagonal_imag = broadening[0] * identity
    couplings = jax.vmap(jnp.diag)(hop_strength) + hop_mixing
    empty_block = jnp.zeros((orbitals, orbitals), jnp.float32)

    def sweep_forward(carried, inputs):
        previous_real, previous_imag, coupling = carried
        block_real, next_coupling = inputs
        reduced_real = block_real - real_product(real_product(coupling.T, previous_real), coupling)
        reduced_imag = diagonal_imag - real_product(real_product(coupling.T, previous_imag), coupling)
        connected = invert_exact(reduced_real, reduced_imag)
        return ((connected[0], connected[1], next_coupling), connected)
    ending, connected = lax.scan(sweep_forward, (empty_block, empty_block, empty_block), (diagonal_real, couplings))

    def sweep_backward(following, inputs):
        here_real, here_imag, coupling = inputs
        left_side = (real_product(here_real, coupling), real_product(here_imag, coupling))
        middle = complex_product(left_side, following)
        right_side = (real_product(middle[0], coupling.T), real_product(middle[1], coupling.T))
        correction = complex_product(right_side, (here_real, here_imag))
        result = (here_real + correction[0], here_imag + correction[1])
        return (result, result)
    final_block = (connected[0][-1], connected[1][-1])
    leftover, earlier = lax.scan(sweep_backward, final_block, (connected[0][:-1], connected[1][:-1], couplings[:-1]), reverse=True)
    green_real = jnp.concatenate([earlier[0], final_block[0][None]], axis=0)
    green_imag = jnp.concatenate([earlier[1], final_block[1][None]], axis=0)
    return (green_real, green_imag)
```

```python
import functools

import jax
import jax.numpy as jnp
from jax import lax
from jax.experimental import pallas as pl
from jax.experimental.pallas import tpu as pltpu
from jax.sharding import PartitionSpec as P

TILE = 8


def dot(first, second, precision=lax.Precision.HIGHEST):
    return jnp.dot(first, second, precision=precision, preferred_element_type=jnp.float32)


def product(first, second, precision=lax.Precision.HIGHEST):
    columns = second[0].shape[1]
    left = jnp.concatenate([first[0], first[1]], axis=1)
    right = jnp.concatenate(
        [
            jnp.concatenate([second[0], second[1]], axis=1),
            jnp.concatenate([-second[1], second[0]], axis=1),
        ],
        axis=0,
    )
    out = dot(left, right, precision)
    return (out[:, :columns], out[:, columns:])


def flipped(block):
    return (block[0].T, block[1].T)


def rows(*blocks):
    return tuple(jnp.concatenate([b[part] for b in blocks], axis=0) for part in (0, 1))


def cols(*blocks):
    return tuple(jnp.concatenate([b[part] for b in blocks], axis=1) for part in (0, 1))


def chosen(flag, first, second):
    return tuple(jnp.where(flag, a, b) for a, b in zip(first, second))


def read(ref, *index):
    return (ref[(*index[:-1], index[-1])], ref[(*index[:-1], index[-1] + 1)])


def write(ref, block, *index):
    ref[(*index[:-1], index[-1])] = block[0]
    ref[(*index[:-1], index[-1] + 1)] = block[1]


def eye(size):
    row = lax.broadcasted_iota(jnp.int32, (size, size), 0)
    column = lax.broadcasted_iota(jnp.int32, (size, size), 1)
    return row == column


def times(a, b):
    return (a[0] * b[0] - a[1] * b[1], a[0] * b[1] + a[1] * b[0])

def plus(a, b):
    return (a[0] + b[0], a[1] + b[1])

def minus(a, b):
    return (a[0] - b[0], a[1] - b[1])

def total(terms):
    while len(terms) > 1:
        terms = [plus(*terms[i : i + 2]) if i + 1 < len(terms) else terms[i] for i in range(0, len(terms), 2)]
    return terms[0]

def pick(flag, value, block):
    return (jnp.where(flag, value, block[0]), jnp.where(flag, 0.0, block[1]))

def sweep(rows, tile, panel, lane, sub):
    size = lane.shape[1]
    first = TILE * tile
    def column(block, j):
        at = first + j
        index = jnp.full((TILE, size), at, jnp.int32)
        return tuple(jnp.take_along_axis(b, index, axis=1) for b in block)
    def row(block, j):
        return tuple(jnp.broadcast_to(b[j : j + 1], (TILE, size)) for b in block)
    own = rows[tile]
    columns = [column(own, j) for j in range(TILE)]
    others = [v for v in panel if v != tile]
    if tile + 1 in others:
        others.remove(tile + 1); others.insert(0, tile + 1)
    sides = {v: [column(rows[v], j) for j in range(TILE)] for v in others}
    inside = (lane >= first) & (lane < first + TILE)
    unit = jnp.where(lane - first == sub, 1.0, 0.0)
    own = pick(inside, unit, own)
    for p in range(0, TILE, 2):
        low, high = columns[p], columns[p + 1]
        a, b, d = row(low, p), row(high, p), row(high, p + 1)
        det = minus(times(a, d), times(b, b))
        scale = 1.0 / (det[0] * det[0] + det[1] * det[1])
        q = (det[0] * scale, -det[1] * scale)
        at_low, at_high = sub == p, sub == p + 1
        here = at_low | at_high
        low = pick(at_high, 0.0, pick(at_low, -1.0, low))
        high = pick(at_low, 0.0, pick(at_high, -1.0, high))
        e_low = minus(times(low, d), times(high, b))
        e_high = minus(times(high, a), times(low, b))
        d_low, d_high = times(e_low, q), times(e_high, q)
        for j in range(p + 2, TILE):
            old = columns[j]
            up, down = row(old, p), row(old, p + 1)
            kept = pick(here, 0.0, old)
            if j < p + 4:
                change = times(plus(times(e_low, up), times(e_high, down)), q)
            else:
                change = plus(times(d_low, up), times(d_high, down))
            columns[j] = minus(kept, change)
        up, down = row(own, p), row(own, p + 1)
        own = minus(pick(here, 0.0, own), plus(times(d_low, up), times(d_high, down)))
    rows[tile] = own
    spread = [row(own, j) for j in range(TILE)]
    for v in others:
        change = total([times(sides[v][j], spread[j]) for j in range(TILE)])
        rows[v] = minus(pick(inside, 0.0, rows[v]), change)

def inverse(block, parts=4, ahead=2):
    size = block[0].shape[0]
    lane = lax.broadcasted_iota(jnp.int32, (TILE, size), 1)
    sub = lax.broadcasted_iota(jnp.int32, (TILE, size), 0)
    count = size // TILE
    rows = [tuple(b[TILE * v : TILE * v + TILE] for b in block) for v in range(count)]
    step = count // parts
    def stack(which):
        return tuple(jnp.concatenate([rows[v][c] for v in which], axis=0) for c in (0, 1))
    for h in range(parts):
        panel = list(range(h * step, h * step + step))
        ready = [v for v in range(panel[-1] + 1, min(panel[-1] + 1 + ahead, count))]
        rest = [v for v in range(count) if v not in panel + ready]
        start = {v: rows[v] for v in rest}
        for tile in panel:
            sweep(rows, tile, panel + ready, lane, sub)
        if not rest:
            break
        real, imag = stack(panel)
        def pad(x):
            out = []
            if h: out.append(jnp.zeros((h * step * TILE, size), jnp.float32))
            out.append(x)
            if h + 1 < parts: out.append(jnp.zeros(((parts - 1 - h) * step * TILE, size), jnp.float32))
            return jnp.concatenate(out, axis=0)
        right = jnp.concatenate([jnp.concatenate([pad(real), pad(imag)], axis=1), jnp.concatenate([pad(-imag), pad(real)], axis=1)], axis=0)
        left = jnp.concatenate(list(stack(rest)), axis=1)
        out = dot(left, right)
        gone = (lane >= h * step * TILE) & (lane < (h + 1) * step * TILE)
        for n, v in enumerate(rest):
            part = out[TILE * n : TILE * n + TILE]
            rows[v] = minus(pick(gone, 0.0, rows[v]), (part[:, :size], part[:, size:]))
    return stack(range(count))


def pack(block, row, column):
    diagonal = jnp.sum(jnp.where(row == column, block[1], 0.0), axis=0, keepdims=True)
    return jnp.concatenate(
        [jnp.where(row <= column, block[0], block[1]), jnp.broadcast_to(diagonal, (TILE, block[0].shape[1]))],
        axis=0,
    )


def unpack(packed, row, column):
    size = packed.shape[1]
    block = packed[:size]
    mirror = block.T
    diagonal = packed[size : size + 1]
    return (
        jnp.where(row <= column, block, mirror),
        jnp.where(row == column, diagonal, jnp.where(row > column, block, mirror)),
    )


def wire(count, energy_ref, broad_ref, onsite_ref, mix_ref, hop_ref, hopmix_ref, real_ref, imag_ref,
         crit_out, crit_in, rest_out, rest_in, own_ref, crit_sent, crit_got, rest_sent, rest_got):
    levels = count.bit_length() - 1
    last = levels - 1
    size = mix_ref.shape[1]
    me = lax.axis_index("slab")
    row = lax.broadcasted_iota(jnp.int32, (size, size), 0)
    column = lax.broadcasted_iota(jnp.int32, (size, size), 1)

    def bit(stride):
        return (me // stride) % 2

    def partner(stride):
        return me + stride - 2 * stride * bit(stride)

    def copy(level, stride, out, into, sent, got):
        return pltpu.make_async_remote_copy(
            src_ref=out.at[level], dst_ref=into.at[level], send_sem=sent.at[level],
            recv_sem=got.at[level], device_id={"slab": partner(stride)},
            device_id_type=pl.DeviceIdType.MESH,
        )

    def crit(level, stride):
        return copy(level, stride, crit_out, crit_in, crit_sent, crit_got)

    def rest(level, stride):
        return copy(level, stride, rest_out, rest_in, rest_sent, rest_got)

    def write_rest(level, link, end):
        rest_out[level, :size] = link[0]
        rest_out[level, size : 2 * size] = link[1]
        rest_out[level, 2 * size :] = end

    def link_of(ref, level):
        return (ref[level, :size], ref[level, size : 2 * size])

    barrier = pltpu.get_barrier_semaphore()
    for level in range(levels):
        pl.semaphore_signal(
            barrier, inc=1, device_id={"slab": partner(1 << level)},
            device_id_type=pl.DeviceIdType.MESH,
        )

    unit = row == column
    diagonal_i = jnp.where(unit, broad_ref[0], 0.0)

    def onsite(k):
        mixing = mix_ref[k]
        diagonal = jnp.where(unit, energy_ref[0] - onsite_ref[k : k + 1, :], 0.0)
        return diagonal - 0.5 * (mixing + mixing.T)

    def coupling(k):
        return jnp.where(unit, hop_ref[k : k + 1, :], 0.0) + hopmix_ref[k]

    def halves(out):
        return (out[:, :size], out[:, size:])

    middle = inverse((onsite(1), diagonal_i))
    lower = coupling(0)
    upper = jnp.where(me == count - 1, 0.0, coupling(1))
    lower_t, upper_t = lower.T, upper.T
    high = bit(1) > 0
    both = jnp.concatenate([middle[0], middle[1]], axis=0)
    first = jnp.where(high, lower_t, upper)
    weighted = dot(both, first)
    near = (weighted[:size], weighted[size:])
    outs = halves(dot(jnp.where(high, lower, upper_t), jnp.concatenate(near, axis=1)))
    alpha = pack((onsite(0), diagonal_i), row, column)
    change = pack(outs, row, column)
    crit_out[0] = jnp.where(high, alpha - change, change)
    pl.semaphore_wait(barrier, levels)
    if levels > 1:
        crit(0, 1).start()
    weighted = dot(both, jnp.where(high, upper, lower_t))
    far = (weighted[:size], weighted[size:])
    to_low, to_high = chosen(high, near, far), chosen(high, far, near)
    outs = halves(dot(jnp.where(high, upper_t, lower), jnp.concatenate(far, axis=1)))
    link = halves(dot(lower, jnp.concatenate(to_high, axis=1)))
    change = pack(outs, row, column)
    write_rest(0, link, jnp.where(high, change, alpha - change))
    if levels > 1:
        rest(0, 1).start()
    zero = jnp.zeros((size, size), jnp.float32)
    one = jnp.where(unit, 1.0, 0.0)
    write(own_ref, (zero, zero), 0, 0)
    write(own_ref, (one, zero), 0, 2)
    write(own_ref, (zero, zero), 0, 4)
    write(own_ref, middle, 1, 0)
    write(own_ref, to_low, 1, 2)
    write(own_ref, to_high, 1, 4)

    def eliminated(level, high):
        packed = jnp.where(high, 1.0, -1.0) * (crit_out[level] - crit_in[level])
        return inverse(unpack(packed, row, column))

    def step(level, stride):
        high = bit(stride) > 0
        crit(level, stride).wait_recv()
        y = eliminated(level, high)
        rest(level, stride).wait_recv()
        mine, other = link_of(rest_out, level), link_of(rest_in, level)
        low_link, high_link = chosen(high, other, mine), chosen(high, mine, other)
        mine, other = rest_out[level, 2 * size :], rest_in[level, 2 * size :]
        alpha, beta = jnp.where(high, other, mine), jnp.where(high, mine, other)
        low_t, high_t = flipped(low_link), flipped(high_link)
        following = bit(2 * stride) > 0
        near = product(chosen(following, low_link, high_t), y)
        change = pack(product(near, chosen(following, low_t, high_link)), row, column)
        crit_out[level + 1] = jnp.where(following, alpha - change, beta + change)

        @pl.when(level + 1 < last)
        def _():
            crit(level + 1, 2 * stride).start()

        far = product(chosen(following, high_t, low_link), y)
        change = pack(product(far, chosen(following, high_link, low_t)), row, column)
        link = product(chosen(following, near, far), high_link)
        write_rest(level + 1, link, jnp.where(following, beta + change, alpha - change))

        @pl.when(level + 1 < last)
        def _():
            rest(level + 1, 2 * stride).start()

        legs = cols(low_t, high_link)
        states = [[read(own_ref, k, 2 * piece) for piece in range(3)] for k in range(2)]
        used = [chosen(high, state[1], state[2]) for state in states]
        weighted = product(rows(*used), y)
        moved = product(weighted, legs)
        for k, state in enumerate(states):
            part = slice(k * size, (k + 1) * size)
            own = product((weighted[0][part], weighted[1][part]), flipped(used[k]))
            write(own_ref, tuple(s + o for s, o in zip(state[0], own)), k, 0)
            down = tuple(
                jnp.where(high, 0.0, s) + m[part, :size] for s, m in zip(state[1], moved)
            )
            up = tuple(
                jnp.where(high, s, 0.0) + m[part, size:] for s, m in zip(state[2], moved)
            )
            write(own_ref, down, k, 2)
            write(own_ref, up, k, 4)
        return 2 * stride

    stride = lax.fori_loop(0, last, step, jnp.int32(1))
    high = bit(stride) > 0
    mine, end = crit_out[last], rest_out[last, 2 * size :]
    link = link_of(rest_out, last)
    ground = inverse(unpack(jnp.where(high, mine, end), row, column))
    change = pack(product(product(flipped(link), ground), link), row, column)
    crit_out[last] = jnp.where(high, mine, mine + change)
    crit(last, stride).start()
    states = [[read(own_ref, k, 2 * piece) for piece in range(3)] for k in range(2)]
    weighted = product(rows(*(state[1] for state in states)), ground)
    moved = product(weighted, link)
    owns, legs = [], []
    for k, state in enumerate(states):
        part = slice(k * size, (k + 1) * size)
        own = product((weighted[0][part], weighted[1][part]), flipped(state[1]))
        owns.append(tuple(s + jnp.where(high, 0.0, o) for s, o in zip(state[0], own)))
        legs.append(
            tuple(jnp.where(high, d, u + m[part]) for d, u, m in zip(state[1], state[2], moved))
        )
    crit(last, stride).wait_recv()
    y = eliminated(last, high)
    weighted = product(rows(*legs), y)
    for k in range(2):
        part = slice(k * size, (k + 1) * size)
        out = product((weighted[0][part], weighted[1][part]), flipped(legs[k]))
        real_ref[k] = owns[k][0] + out[0]
        imag_ref[k] = owns[k][1] + out[1]

    def drain(level, stride):
        crit(level, stride).wait_send()
        rest(level, stride).wait_send()
        return 2 * stride

    stride = lax.fori_loop(0, last, drain, jnp.int32(1))
    crit(last, stride).wait_send()


def shards(onsite_energy, onsite_mixing, hop_strength, hop_mixing, energy, broadening):
    size = onsite_mixing.shape[1]
    count = lax.axis_size("slab")
    levels = count.bit_length() - 1
    vmem = pl.BlockSpec(memory_space=pltpu.VMEM)
    smem = pl.BlockSpec(memory_space=pltpu.SMEM)
    out = jax.ShapeDtypeStruct(onsite_mixing.shape, jnp.float32)
    crit = pltpu.VMEM((levels, size + TILE, size), jnp.float32)
    rest = pltpu.VMEM((levels, 3 * size + TILE, size), jnp.float32)
    return pl.pallas_call(
        functools.partial(wire, count),
        out_shape=[out, out],
        in_specs=[smem] * 2 + [vmem] * 4,
        out_specs=[vmem, vmem],
        scratch_shapes=[crit, crit, rest, rest, pltpu.VMEM((2, 6, size, size), jnp.float32)]
        + [pltpu.SemaphoreType.DMA((levels,))] * 4,
        compiler_params=pltpu.CompilerParams(collective_id=0, has_side_effects=True),
        name="wire",
    )(energy, broadening, onsite_energy, onsite_mixing, hop_strength, hop_mixing)


def solution(mesh):
    return jax.shard_map(
        shards,
        mesh=mesh,
        in_specs=(
            P("slab", None),
            P("slab", None, None),
            P("slab", None),
            P("slab", None, None),
            P("energy"),
            P("energy"),
        ),
        out_specs=(P(("energy", "slab"), None, None), P(("energy", "slab"), None, None)),
        check_vma=False,
    )
```

```python
import functools

import jax
import jax.numpy as jnp
from jax import lax
from jax.experimental import pallas as pl
from jax.experimental.pallas import tpu as pltpu
from jax.sharding import PartitionSpec as P

TILE = 8


def dot(first, second, precision=lax.Precision.HIGHEST):
    return jnp.dot(first, second, precision=precision, preferred_element_type=jnp.float32)


def product(first, second, precision=lax.Precision.HIGHEST):
    columns = second[0].shape[1]
    left = jnp.concatenate([first[0], first[1]], axis=1)
    right = jnp.concatenate(
        [
            jnp.concatenate([second[0], second[1]], axis=1),
            jnp.concatenate([-second[1], second[0]], axis=1),
        ],
        axis=0,
    )
    out = dot(left, right, precision)
    return (out[:, :columns], out[:, columns:])


def flipped(block):
    return (block[0].T, block[1].T)


def rows(*blocks):
    return tuple(jnp.concatenate([b[part] for b in blocks], axis=0) for part in (0, 1))


def cols(*blocks):
    return tuple(jnp.concatenate([b[part] for b in blocks], axis=1) for part in (0, 1))


def chosen(flag, first, second):
    return tuple(jnp.where(flag, a, b) for a, b in zip(first, second))


def read(ref, *index):
    return (ref[(*index[:-1], index[-1])], ref[(*index[:-1], index[-1] + 1)])


def write(ref, block, *index):
    ref[(*index[:-1], index[-1])] = block[0]
    ref[(*index[:-1], index[-1] + 1)] = block[1]


def eye(size):
    row = lax.broadcasted_iota(jnp.int32, (size, size), 0)
    column = lax.broadcasted_iota(jnp.int32, (size, size), 1)
    return row == column


def times(a, b):
    return (a[0] * b[0] - a[1] * b[1], a[0] * b[1] + a[1] * b[0])

def plus(a, b):
    return (a[0] + b[0], a[1] + b[1])

def minus(a, b):
    return (a[0] - b[0], a[1] - b[1])

def total(terms):
    while len(terms) > 1:
        terms = [plus(*terms[i : i + 2]) if i + 1 < len(terms) else terms[i] for i in range(0, len(terms), 2)]
    return terms[0]

def pick(flag, value, block):
    return (jnp.where(flag, value, block[0]), jnp.where(flag, 0.0, block[1]))

def sweep(rows, tile, panel, lane, sub):
    size = lane.shape[1]
    first = TILE * tile
    def column(block, j):
        at = first + j
        index = jnp.full((TILE, size), at, jnp.int32)
        return tuple(jnp.take_along_axis(b, index, axis=1) for b in block)
    def row(block, j):
        return tuple(jnp.broadcast_to(b[j : j + 1], (TILE, size)) for b in block)
    own = rows[tile]
    columns = [column(own, j) for j in range(TILE)]
    others = [v for v in panel if v != tile]
    if tile + 1 in others:
        others.remove(tile + 1); others.insert(0, tile + 1)
    sides = {v: [column(rows[v], j) for j in range(TILE)] for v in others}
    inside = (lane >= first) & (lane < first + TILE)
    unit = jnp.where(lane - first == sub, 1.0, 0.0)
    own = pick(inside, unit, own)
    for p in range(0, TILE, 2):
        low, high = columns[p], columns[p + 1]
        a, b, d = row(low, p), row(high, p), row(high, p + 1)
        det = minus(times(a, d), times(b, b))
        scale = 1.0 / (det[0] * det[0] + det[1] * det[1])
        q = (det[0] * scale, -det[1] * scale)
        at_low, at_high = sub == p, sub == p + 1
        here = at_low | at_high
        low = pick(at_high, 0.0, pick(at_low, -1.0, low))
        high = pick(at_low, 0.0, pick(at_high, -1.0, high))
        e_low = minus(times(low, d), times(high, b))
        e_high = minus(times(high, a), times(low, b))
        d_low, d_high = times(e_low, q), times(e_high, q)
        for j in range(p + 2, TILE):
            old = columns[j]
            up, down = row(old, p), row(old, p + 1)
            kept = pick(here, 0.0, old)
            change = plus(times(d_low, up), times(d_high, down))
            columns[j] = minus(kept, change)
        up, down = row(own, p), row(own, p + 1)
        own = minus(pick(here, 0.0, own), plus(times(d_low, up), times(d_high, down)))
    rows[tile] = own
    spread = [row(own, j) for j in range(TILE)]
    for v in others:
        change = total([times(sides[v][j], spread[j]) for j in range(TILE)])
        rows[v] = minus(pick(inside, 0.0, rows[v]), change)

def inverse(block, parts=4, ahead=2):
    size = block[0].shape[0]
    lane = lax.broadcasted_iota(jnp.int32, (TILE, size), 1)
    sub = lax.broadcasted_iota(jnp.int32, (TILE, size), 0)
    count = size // TILE
    step = count // parts
    width = step * TILE

    def trip(_, carried):
        rows = [tuple(b[TILE * v : TILE * v + TILE] for b in carried) for v in range(count)]
        ready = list(range(step, step + ahead))
        rest = list(range(step + ahead, count))
        left = jnp.concatenate([carried[0][width + ahead * TILE :], carried[1][width + ahead * TILE :]], axis=1)
        for tile in range(step):
            sweep(rows, tile, list(range(step)) + ready, lane, sub)
        empty = jnp.zeros((size - width, 2 * size), jnp.float32)
        real, imag = (jnp.concatenate([rows[v][c] for v in range(step)], axis=0) for c in (0, 1))
        right = jnp.concatenate(
            [jnp.concatenate([real, imag], axis=1), empty, jnp.concatenate([-imag, real], axis=1), empty], axis=0
        )
        out = dot(left, right)
        gone = lane < width
        for n, v in enumerate(rest):
            part = out[TILE * n : TILE * n + TILE]
            rows[v] = minus(pick(gone, 0.0, rows[v]), (part[:, :size], part[:, size:]))
        order = list(range(step, count)) + list(range(step))
        return tuple(
            pltpu.roll(jnp.concatenate([rows[v][c] for v in order], axis=0), size - width, 1) for c in (0, 1)
        )

    return lax.fori_loop(0, parts, trip, block)


def pack(block, row, column):
    diagonal = jnp.sum(jnp.where(row == column, block[1], 0.0), axis=0, keepdims=True)
    return jnp.concatenate(
        [jnp.where(row <= column, block[0], block[1]), jnp.broadcast_to(diagonal, (TILE, block[0].shape[1]))],
        axis=0,
    )


def unpack(packed, row, column):
    size = packed.shape[1]
    block = packed[:size]
    mirror = block.T
    diagonal = packed[size : size + 1]
    return (
        jnp.where(row <= column, block, mirror),
        jnp.where(row == column, diagonal, jnp.where(row > column, block, mirror)),
    )


def wire(count, energy_ref, broad_ref, onsite_ref, mix_ref, hop_ref, hopmix_ref, real_ref, imag_ref,
         crit_out, crit_in, rest_out, rest_in, own_ref, crit_sent, crit_got, rest_sent, rest_got):
    levels = count.bit_length() - 1
    last = levels - 1
    size = mix_ref.shape[1]
    me = lax.axis_index("slab")
    row = lax.broadcasted_iota(jnp.int32, (size, size), 0)
    column = lax.broadcasted_iota(jnp.int32, (size, size), 1)

    def bit(stride):
        return (me // stride) % 2

    def partner(stride):
        return me + stride - 2 * stride * bit(stride)

    def copy(level, stride, out, into, sent, got):
        return pltpu.make_async_remote_copy(
            src_ref=out.at[level], dst_ref=into.at[level], send_sem=sent.at[level],
            recv_sem=got.at[level], device_id={"slab": partner(stride)},
            device_id_type=pl.DeviceIdType.MESH,
        )

    def crit(level, stride):
        return copy(level, stride, crit_out, crit_in, crit_sent, crit_got)

    def rest(level, stride):
        return copy(level, stride, rest_out, rest_in, rest_sent, rest_got)

    def write_rest(level, link, end):
        rest_out[level, :size] = link[0]
        rest_out[level, size : 2 * size] = link[1]
        rest_out[level, 2 * size :] = end

    def link_of(ref, level):
        return (ref[level, :size], ref[level, size : 2 * size])

    barrier = pltpu.get_barrier_semaphore()
    for level in range(levels):
        pl.semaphore_signal(
            barrier, inc=1, device_id={"slab": partner(1 << level)},
            device_id_type=pl.DeviceIdType.MESH,
        )

    unit = row == column
    diagonal_i = jnp.where(unit, broad_ref[0], 0.0)

    def onsite(k):
        mixing = mix_ref[k]
        diagonal = jnp.where(unit, energy_ref[0] - onsite_ref[k : k + 1, :], 0.0)
        return diagonal - 0.5 * (mixing + mixing.T)

    def coupling(k):
        return jnp.where(unit, hop_ref[k : k + 1, :], 0.0) + hopmix_ref[k]

    def halves(out):
        return (out[:, :size], out[:, size:])

    middle = inverse((onsite(1), diagonal_i))
    lower = coupling(0)
    upper = jnp.where(me == count - 1, 0.0, coupling(1))
    lower_t, upper_t = lower.T, upper.T
    high = bit(1) > 0
    both = jnp.concatenate([middle[0], middle[1]], axis=0)
    first = jnp.where(high, lower_t, upper)
    weighted = dot(both, first)
    near = (weighted[:size], weighted[size:])
    outs = halves(dot(jnp.where(high, lower, upper_t), jnp.concatenate(near, axis=1)))
    alpha = pack((onsite(0), diagonal_i), row, column)
    change = pack(outs, row, column)
    crit_out[0] = jnp.where(high, alpha - change, change)
    pl.semaphore_wait(barrier, levels)
    if levels > 1:
        crit(0, 1).start()
    weighted = dot(both, jnp.where(high, upper, lower_t))
    far = (weighted[:size], weighted[size:])
    to_low, to_high = chosen(high, near, far), chosen(high, far, near)
    outs = halves(dot(jnp.where(high, upper_t, lower), jnp.concatenate(far, axis=1)))
    link = halves(dot(lower, jnp.concatenate(to_high, axis=1)))
    change = pack(outs, row, column)
    write_rest(0, link, jnp.where(high, change, alpha - change))
    if levels > 1:
        rest(0, 1).start()
    zero = jnp.zeros((size, size), jnp.float32)
    one = jnp.where(unit, 1.0, 0.0)
    write(own_ref, (zero, zero), 0, 0)
    write(own_ref, (one, zero), 0, 2)
    write(own_ref, (zero, zero), 0, 4)
    write(own_ref, middle, 1, 0)
    write(own_ref, to_low, 1, 2)
    write(own_ref, to_high, 1, 4)

    def eliminated(level, high):
        packed = jnp.where(high, 1.0, -1.0) * (crit_out[level] - crit_in[level])
        return inverse(unpack(packed, row, column))

    def step(level, stride):
        high = bit(stride) > 0
        crit(level, stride).wait_recv()
        y = eliminated(level, high)
        rest(level, stride).wait_recv()
        mine, other = link_of(rest_out, level), link_of(rest_in, level)
        low_link, high_link = chosen(high, other, mine), chosen(high, mine, other)
        mine, other = rest_out[level, 2 * size :], rest_in[level, 2 * size :]
        alpha, beta = jnp.where(high, other, mine), jnp.where(high, mine, other)
        low_t, high_t = flipped(low_link), flipped(high_link)
        following = bit(2 * stride) > 0
        near = product(chosen(following, low_link, high_t), y)
        change = pack(product(near, chosen(following, low_t, high_link)), row, column)
        crit_out[level + 1] = jnp.where(following, alpha - change, beta + change)

        @pl.when(level + 1 < last)
        def _():
            crit(level + 1, 2 * stride).start()

        far = product(chosen(following, high_t, low_link), y)
        change = pack(product(far, chosen(following, high_link, low_t)), row, column)
        link = product(chosen(following, near, far), high_link)
        write_rest(level + 1, link, jnp.where(following, beta + change, alpha - change))

        @pl.when(level + 1 < last)
        def _():
            rest(level + 1, 2 * stride).start()

        legs = cols(low_t, high_link)
        states = [[read(own_ref, k, 2 * piece) for piece in range(3)] for k in range(2)]
        used = [chosen(high, state[1], state[2]) for state in states]
        weighted = product(rows(*used), y)
        moved = product(weighted, legs)
        for k, state in enumerate(states):
            part = slice(k * size, (k + 1) * size)
            own = product((weighted[0][part], weighted[1][part]), flipped(used[k]))
            write(own_ref, tuple(s + o for s, o in zip(state[0], own)), k, 0)
            down = tuple(
                jnp.where(high, 0.0, s) + m[part, :size] for s, m in zip(state[1], moved)
            )
            up = tuple(
                jnp.where(high, s, 0.0) + m[part, size:] for s, m in zip(state[2], moved)
            )
            write(own_ref, down, k, 2)
            write(own_ref, up, k, 4)
        return 2 * stride

    stride = lax.fori_loop(0, last, step, jnp.int32(1))
    high = bit(stride) > 0
    mine, end = crit_out[last], rest_out[last, 2 * size :]
    link = link_of(rest_out, last)
    ground = inverse(unpack(jnp.where(high, mine, end), row, column))
    change = pack(product(product(flipped(link), ground), link), row, column)
    crit_out[last] = jnp.where(high, mine, mine + change)
    crit(last, stride).start()
    states = [[read(own_ref, k, 2 * piece) for piece in range(3)] for k in range(2)]
    weighted = product(rows(*(state[1] for state in states)), ground)
    moved = product(weighted, link)
    owns, legs = [], []
    for k, state in enumerate(states):
        part = slice(k * size, (k + 1) * size)
        own = product((weighted[0][part], weighted[1][part]), flipped(state[1]))
        owns.append(tuple(s + jnp.where(high, 0.0, o) for s, o in zip(state[0], own)))
        legs.append(
            tuple(jnp.where(high, d, u + m[part]) for d, u, m in zip(state[1], state[2], moved))
        )
    crit(last, stride).wait_recv()
    y = eliminated(last, high)
    weighted = product(rows(*legs), y)
    for k in range(2):
        part = slice(k * size, (k + 1) * size)
        out = product((weighted[0][part], weighted[1][part]), flipped(legs[k]))
        real_ref[k] = owns[k][0] + out[0]
        imag_ref[k] = owns[k][1] + out[1]

    def drain(level, stride):
        crit(level, stride).wait_send()
        rest(level, stride).wait_send()
        return 2 * stride

    stride = lax.fori_loop(0, last, drain, jnp.int32(1))
    crit(last, stride).wait_send()


def shards(onsite_energy, onsite_mixing, hop_strength, hop_mixing, energy, broadening):
    size = onsite_mixing.shape[1]
    count = lax.axis_size("slab")
    levels = count.bit_length() - 1
    vmem = pl.BlockSpec(memory_space=pltpu.VMEM)
    smem = pl.BlockSpec(memory_space=pltpu.SMEM)
    out = jax.ShapeDtypeStruct(onsite_mixing.shape, jnp.float32)
    crit = pltpu.VMEM((levels, size + TILE, size), jnp.float32)
    rest = pltpu.VMEM((levels, 3 * size + TILE, size), jnp.float32)
    return pl.pallas_call(
        functools.partial(wire, count),
        out_shape=[out, out],
        in_specs=[smem] * 2 + [vmem] * 4,
        out_specs=[vmem, vmem],
        scratch_shapes=[crit, crit, rest, rest, pltpu.VMEM((2, 6, size, size), jnp.float32)]
        + [pltpu.SemaphoreType.DMA((levels,))] * 4,
        compiler_params=pltpu.CompilerParams(collective_id=0, has_side_effects=True),
        name="wire",
    )(energy, broadening, onsite_energy, onsite_mixing, hop_strength, hop_mixing)


def solution(mesh):
    return jax.shard_map(
        shards,
        mesh=mesh,
        in_specs=(
            P("slab", None),
            P("slab", None, None),
            P("slab", None),
            P("slab", None, None),
            P("energy"),
            P("energy"),
        ),
        out_specs=(P(("energy", "slab"), None, None), P(("energy", "slab"), None, None)),
        check_vma=False,
    )
```

```python
import functools

import jax
import jax.numpy as jnp
from jax import lax
from jax.experimental import pallas as pl
from jax.experimental.pallas import tpu as pltpu
from jax.sharding import PartitionSpec as P

TILE = 8


def dot(first, second, precision=lax.Precision.HIGHEST):
    return jnp.dot(first, second, precision=precision, preferred_element_type=jnp.float32)


def product(first, second, precision=lax.Precision.HIGHEST):
    columns = second[0].shape[1]
    left = jnp.concatenate([first[0], first[1]], axis=1)
    right = jnp.concatenate(
        [
            jnp.concatenate([second[0], second[1]], axis=1),
            jnp.concatenate([-second[1], second[0]], axis=1),
        ],
        axis=0,
    )
    out = dot(left, right, precision)
    return (out[:, :columns], out[:, columns:])


def flipped(block):
    return (block[0].T, block[1].T)


def rows(*blocks):
    return tuple(jnp.concatenate([b[part] for b in blocks], axis=0) for part in (0, 1))


def cols(*blocks):
    return tuple(jnp.concatenate([b[part] for b in blocks], axis=1) for part in (0, 1))


def chosen(flag, first, second):
    return tuple(jnp.where(flag, a, b) for a, b in zip(first, second))


def read(ref, *index):
    return (ref[(*index[:-1], index[-1])], ref[(*index[:-1], index[-1] + 1)])


def write(ref, block, *index):
    ref[(*index[:-1], index[-1])] = block[0]
    ref[(*index[:-1], index[-1] + 1)] = block[1]


def eye(size):
    row = lax.broadcasted_iota(jnp.int32, (size, size), 0)
    column = lax.broadcasted_iota(jnp.int32, (size, size), 1)
    return row == column


def times(a, b):
    return (a[0] * b[0] - a[1] * b[1], a[0] * b[1] + a[1] * b[0])

def plus(a, b):
    return (a[0] + b[0], a[1] + b[1])

def minus(a, b):
    return (a[0] - b[0], a[1] - b[1])

def total(terms):
    while len(terms) > 1:
        terms = [plus(*terms[i : i + 2]) if i + 1 < len(terms) else terms[i] for i in range(0, len(terms), 2)]
    return terms[0]

def pick(flag, value, block):
    return (jnp.where(flag, value, block[0]), jnp.where(flag, 0.0, block[1]))

def sweep(rows, tile, panel, lane, sub):
    size = lane.shape[1]
    first = TILE * tile
    def column(block, j):
        at = first + j
        index = jnp.full((TILE, size), at, jnp.int32)
        return tuple(jnp.take_along_axis(b, index, axis=1) for b in block)
    def row(block, j):
        return tuple(jnp.broadcast_to(b[j : j + 1], (TILE, size)) for b in block)
    own = rows[tile]
    columns = [column(own, j) for j in range(TILE)]
    others = [v for v in panel if v != tile]
    if tile + 1 in others:
        others.remove(tile + 1); others.insert(0, tile + 1)
    sides = {v: [column(rows[v], j) for j in range(TILE)] for v in others}
    inside = (lane >= first) & (lane < first + TILE)
    unit = jnp.where(lane - first == sub, 1.0, 0.0)
    own = pick(inside, unit, own)
    for p in range(0, TILE, 2):
        low, high = columns[p], columns[p + 1]
        a, b, d = row(low, p), row(high, p), row(high, p + 1)
        det = minus(times(a, d), times(b, b))
        scale = 1.0 / (det[0] * det[0] + det[1] * det[1])
        q = (det[0] * scale, -det[1] * scale)
        at_low, at_high = sub == p, sub == p + 1
        here = at_low | at_high
        low = pick(at_high, 0.0, pick(at_low, -1.0, low))
        high = pick(at_low, 0.0, pick(at_high, -1.0, high))
        e_low = minus(times(low, d), times(high, b))
        e_high = minus(times(high, a), times(low, b))
        d_low, d_high = times(e_low, q), times(e_high, q)
        for j in range(p + 2, TILE):
            old = columns[j]
            up, down = row(old, p), row(old, p + 1)
            kept = pick(here, 0.0, old)
            change = plus(times(d_low, up), times(d_high, down))
            columns[j] = minus(kept, change)
        up, down = row(own, p), row(own, p + 1)
        own = minus(pick(here, 0.0, own), plus(times(d_low, up), times(d_high, down)))
    rows[tile] = own
    spread = [row(own, j) for j in range(TILE)]
    for v in others:
        change = total([times(sides[v][j], spread[j]) for j in range(TILE)])
        rows[v] = minus(pick(inside, 0.0, rows[v]), change)

def inverse(block, parts=4, ahead=2):
    size = block[0].shape[0]
    lane = lax.broadcasted_iota(jnp.int32, (TILE, size), 1)
    sub = lax.broadcasted_iota(jnp.int32, (TILE, size), 0)
    count = size // TILE
    step = count // parts
    width = step * TILE

    def trip(_, carried):
        rows = [tuple(b[TILE * v : TILE * v + TILE] for b in carried) for v in range(count)]
        ready = list(range(step, step + ahead))
        rest = list(range(step + ahead, count))
        left = jnp.concatenate([carried[0][width + ahead * TILE :], carried[1][width + ahead * TILE :]], axis=1)
        for tile in range(step):
            sweep(rows, tile, list(range(step)) + ready, lane, sub)
        empty = jnp.zeros((size - width, 2 * size), jnp.float32)
        real, imag = (jnp.concatenate([rows[v][c] for v in range(step)], axis=0) for c in (0, 1))
        right = jnp.concatenate(
            [jnp.concatenate([real, imag], axis=1), empty, jnp.concatenate([-imag, real], axis=1), empty], axis=0
        )
        out = dot(left, right)
        gone = lane < width
        for n, v in enumerate(rest):
            part = out[TILE * n : TILE * n + TILE]
            rows[v] = minus(pick(gone, 0.0, rows[v]), (part[:, :size], part[:, size:]))
        order = list(range(step, count)) + list(range(step))
        return tuple(
            pltpu.roll(jnp.concatenate([rows[v][c] for v in order], axis=0), size - width, 1) for c in (0, 1)
        )

    return lax.fori_loop(0, parts, trip, block)


def pack(block, row, column):
    diagonal = jnp.sum(jnp.where(row == column, block[1], 0.0), axis=0, keepdims=True)
    return jnp.concatenate(
        [jnp.where(row <= column, block[0], block[1]), jnp.broadcast_to(diagonal, (TILE, block[0].shape[1]))],
        axis=0,
    )


def unpack(packed, row, column):
    size = packed.shape[1]
    block = packed[:size]
    mirror = block.T
    diagonal = packed[size : size + 1]
    return (
        jnp.where(row <= column, block, mirror),
        jnp.where(row == column, diagonal, jnp.where(row > column, block, mirror)),
    )


def wire(count, energy_ref, broad_ref, onsite_ref, mix_ref, hop_ref, hopmix_ref, real_ref, imag_ref,
         crit_out, crit_in, rest_out, rest_in, own_ref, kept_ref, crit_sent, crit_got, rest_sent, rest_got):
    levels = count.bit_length() - 1
    last = levels - 1
    size = mix_ref.shape[1]
    me = lax.axis_index("slab")
    row = lax.broadcasted_iota(jnp.int32, (size, size), 0)
    column = lax.broadcasted_iota(jnp.int32, (size, size), 1)

    def bit(stride):
        return (me // stride) % 2

    def partner(stride):
        return me + stride - 2 * stride * bit(stride)

    def copy(level, stride, out, into, sent, got):
        return pltpu.make_async_remote_copy(
            src_ref=out.at[level], dst_ref=into.at[level], send_sem=sent.at[level],
            recv_sem=got.at[level], device_id={"slab": partner(stride)},
            device_id_type=pl.DeviceIdType.MESH,
        )

    def crit(level, stride):
        return copy(level, stride, crit_out, crit_in, crit_sent, crit_got)

    def rest(level, stride):
        return copy(level, stride, rest_out, rest_in, rest_sent, rest_got)

    def write_rest(level, link, end):
        rest_out[level, :size] = link[0]
        rest_out[level, size : 2 * size] = link[1]
        rest_out[level, 2 * size :] = end

    def link_of(ref, level):
        return (ref[level, :size], ref[level, size : 2 * size])

    barrier = pltpu.get_barrier_semaphore()
    for level in range(levels):
        pl.semaphore_signal(
            barrier, inc=1, device_id={"slab": partner(1 << level)},
            device_id_type=pl.DeviceIdType.MESH,
        )

    unit = row == column
    diagonal_i = jnp.where(unit, broad_ref[0], 0.0)

    def onsite(k):
        mixing = mix_ref[k]
        diagonal = jnp.where(unit, energy_ref[0] - onsite_ref[k : k + 1, :], 0.0)
        return diagonal - 0.5 * (mixing + mixing.T)

    def coupling(k):
        return jnp.where(unit, hop_ref[k : k + 1, :], 0.0) + hopmix_ref[k]

    def halves(out):
        return (out[:, :size], out[:, size:])

    middle = inverse((onsite(1), diagonal_i))
    lower = coupling(0)
    upper = jnp.where(me == count - 1, 0.0, coupling(1))
    lower_t, upper_t = lower.T, upper.T
    high = bit(1) > 0
    both = jnp.concatenate([middle[0], middle[1]], axis=0)
    first = jnp.where(high, lower_t, upper)
    weighted = dot(both, first)
    near = (weighted[:size], weighted[size:])
    outs = halves(dot(jnp.where(high, lower, upper_t), jnp.concatenate(near, axis=1)))
    alpha = pack((onsite(0), diagonal_i), row, column)
    change = pack(outs, row, column)
    crit_out[0] = jnp.where(high, alpha - change, change)
    pl.semaphore_wait(barrier, levels)
    if levels > 1:
        crit(0, 1).start()
    weighted = dot(both, jnp.where(high, upper, lower_t))
    far = (weighted[:size], weighted[size:])
    to_low, to_high = chosen(high, near, far), chosen(high, far, near)
    outs = halves(dot(jnp.where(high, upper_t, lower), jnp.concatenate(far, axis=1)))
    link = halves(dot(lower, jnp.concatenate(to_high, axis=1)))
    change = pack(outs, row, column)
    write_rest(0, link, jnp.where(high, change, alpha - change))
    if levels > 1:
        rest(0, 1).start()
    zero = jnp.zeros((size, size), jnp.float32)
    one = jnp.where(unit, 1.0, 0.0)
    write(own_ref, (zero, zero), 0, 0)
    write(own_ref, (one, zero), 0, 2)
    write(own_ref, (zero, zero), 0, 4)
    write(own_ref, middle, 1, 0)
    write(own_ref, to_low, 1, 2)
    write(own_ref, to_high, 1, 4)

    def eliminated(level, high):
        packed = jnp.where(high, 1.0, -1.0) * (crit_out[level] - crit_in[level])
        return inverse(unpack(packed, row, column))

    def advance(high, y, low_t, high_link):
        legs = cols(low_t, high_link)
        states = [[read(own_ref, k, 2 * piece) for piece in range(3)] for k in range(2)]
        used = [chosen(high, state[1], state[2]) for state in states]
        weighted = product(rows(*used), y)
        moved = product(weighted, legs)
        for k, state in enumerate(states):
            part = slice(k * size, (k + 1) * size)
            own = product((weighted[0][part], weighted[1][part]), flipped(used[k]))
            write(own_ref, tuple(s + o for s, o in zip(state[0], own)), k, 0)
            down = tuple(
                jnp.where(high, 0.0, s) + m[part, :size] for s, m in zip(state[1], moved)
            )
            up = tuple(
                jnp.where(high, s, 0.0) + m[part, size:] for s, m in zip(state[2], moved)
            )
            write(own_ref, down, k, 2)
            write(own_ref, up, k, 4)

    def step(level, stride):
        high = bit(stride) > 0
        crit(level, stride).wait_recv()
        y = eliminated(level, high)
        rest(level, stride).wait_recv()
        mine, other = link_of(rest_out, level), link_of(rest_in, level)
        low_link, high_link = chosen(high, other, mine), chosen(high, mine, other)
        mine, other = rest_out[level, 2 * size :], rest_in[level, 2 * size :]
        alpha, beta = jnp.where(high, other, mine), jnp.where(high, mine, other)
        low_t, high_t = flipped(low_link), flipped(high_link)
        following = bit(2 * stride) > 0
        near = product(chosen(following, low_link, high_t), y)
        change = pack(product(near, chosen(following, low_t, high_link)), row, column)
        crit_out[level + 1] = jnp.where(following, alpha - change, beta + change)

        @pl.when(level + 1 < last)
        def _():
            crit(level + 1, 2 * stride).start()

        far = product(chosen(following, high_t, low_link), y)
        change = pack(product(far, chosen(following, high_link, low_t)), row, column)
        link = product(chosen(following, near, far), high_link)
        write_rest(level + 1, link, jnp.where(following, beta + change, alpha - change))

        @pl.when(level + 1 < last)
        def _():
            rest(level + 1, 2 * stride).start()

        kept_ref[0] = y[0]
        kept_ref[1] = y[1]

        @pl.when(level + 1 < last)
        def _():
            advance(high, y, low_t, high_link)

        return 2 * stride

    stride = lax.fori_loop(0, last, step, jnp.int32(1))
    high = bit(stride) > 0
    mine, end = crit_out[last], rest_out[last, 2 * size :]
    link = link_of(rest_out, last)
    ground = inverse(unpack(jnp.where(high, mine, end), row, column))
    change = pack(product(product(flipped(link), ground), link), row, column)
    crit_out[last] = jnp.where(high, mine, mine + change)
    crit(last, stride).start()
    if last > 0:
        before = bit(stride // 2) > 0
        mine, other = link_of(rest_out, last - 1), link_of(rest_in, last - 1)
        low_link, high_link = chosen(before, other, mine), chosen(before, mine, other)
        advance(before, (kept_ref[0], kept_ref[1]), flipped(low_link), high_link)
    states = [[read(own_ref, k, 2 * piece) for piece in range(3)] for k in range(2)]
    weighted = product(rows(*(state[1] for state in states)), ground)
    moved = product(weighted, link)
    owns, legs = [], []
    for k, state in enumerate(states):
        part = slice(k * size, (k + 1) * size)
        own = product((weighted[0][part], weighted[1][part]), flipped(state[1]))
        owns.append(tuple(s + jnp.where(high, 0.0, o) for s, o in zip(state[0], own)))
        legs.append(
            tuple(jnp.where(high, d, u + m[part]) for d, u, m in zip(state[1], state[2], moved))
        )
    crit(last, stride).wait_recv()
    y = eliminated(last, high)
    weighted = product(rows(*legs), y)
    for k in range(2):
        part = slice(k * size, (k + 1) * size)
        out = product((weighted[0][part], weighted[1][part]), flipped(legs[k]))
        real_ref[k] = owns[k][0] + out[0]
        imag_ref[k] = owns[k][1] + out[1]

    def drain(level, stride):
        crit(level, stride).wait_send()
        rest(level, stride).wait_send()
        return 2 * stride

    stride = lax.fori_loop(0, last, drain, jnp.int32(1))
    crit(last, stride).wait_send()


def shards(onsite_energy, onsite_mixing, hop_strength, hop_mixing, energy, broadening):
    size = onsite_mixing.shape[1]
    count = lax.axis_size("slab")
    levels = count.bit_length() - 1
    vmem = pl.BlockSpec(memory_space=pltpu.VMEM)
    smem = pl.BlockSpec(memory_space=pltpu.SMEM)
    out = jax.ShapeDtypeStruct(onsite_mixing.shape, jnp.float32)
    crit = pltpu.VMEM((levels, size + TILE, size), jnp.float32)
    rest = pltpu.VMEM((levels, 3 * size + TILE, size), jnp.float32)
    return pl.pallas_call(
        functools.partial(wire, count),
        out_shape=[out, out],
        in_specs=[smem] * 2 + [vmem] * 4,
        out_specs=[vmem, vmem],
        scratch_shapes=[crit, crit, rest, rest, pltpu.VMEM((2, 6, size, size), jnp.float32), pltpu.VMEM((2, size, size), jnp.float32)]
        + [pltpu.SemaphoreType.DMA((levels,))] * 4,
        compiler_params=pltpu.CompilerParams(collective_id=0, has_side_effects=True),
        name="wire",
    )(energy, broadening, onsite_energy, onsite_mixing, hop_strength, hop_mixing)


def solution(mesh):
    return jax.shard_map(
        shards,
        mesh=mesh,
        in_specs=(
            P("slab", None),
            P("slab", None, None),
            P("slab", None),
            P("slab", None, None),
            P("energy"),
            P("energy"),
        ),
        out_specs=(P(("energy", "slab"), None, None), P(("energy", "slab"), None, None)),
        check_vma=False,
    )
```

```python
import functools

import jax
import jax.numpy as jnp
from jax import lax
from jax.experimental import pallas as pl
from jax.experimental.pallas import tpu as pltpu
from jax.sharding import PartitionSpec as P

TILE = 8


def dot(first, second, precision=lax.Precision.HIGHEST):
    return jnp.dot(first, second, precision=precision, preferred_element_type=jnp.float32)


def product(first, second, precision=lax.Precision.HIGHEST):
    columns = second[0].shape[1]
    left = jnp.concatenate([first[0], first[1]], axis=1)
    right = jnp.concatenate(
        [
            jnp.concatenate([second[0], second[1]], axis=1),
            jnp.concatenate([-second[1], second[0]], axis=1),
        ],
        axis=0,
    )
    out = dot(left, right, precision)
    return (out[:, :columns], out[:, columns:])


def flipped(block):
    return (block[0].T, block[1].T)


def rows(*blocks):
    return tuple(jnp.concatenate([b[part] for b in blocks], axis=0) for part in (0, 1))


def cols(*blocks):
    return tuple(jnp.concatenate([b[part] for b in blocks], axis=1) for part in (0, 1))


def chosen(flag, first, second):
    return tuple(jnp.where(flag, a, b) for a, b in zip(first, second))


def read(ref, *index):
    return (ref[(*index[:-1], index[-1])], ref[(*index[:-1], index[-1] + 1)])


def write(ref, block, *index):
    ref[(*index[:-1], index[-1])] = block[0]
    ref[(*index[:-1], index[-1] + 1)] = block[1]


def eye(size):
    row = lax.broadcasted_iota(jnp.int32, (size, size), 0)
    column = lax.broadcasted_iota(jnp.int32, (size, size), 1)
    return row == column


def times(a, b):
    return (a[0] * b[0] - a[1] * b[1], a[0] * b[1] + a[1] * b[0])

def plus(a, b):
    return (a[0] + b[0], a[1] + b[1])

def minus(a, b):
    return (a[0] - b[0], a[1] - b[1])

def total(terms):
    while len(terms) > 1:
        terms = [plus(*terms[i : i + 2]) if i + 1 < len(terms) else terms[i] for i in range(0, len(terms), 2)]
    return terms[0]

def pick(flag, value, block):
    return (jnp.where(flag, value, block[0]), jnp.where(flag, 0.0, block[1]))

def sweep(rows, tile, panel, lane, sub):
    size = lane.shape[1]
    first = TILE * tile
    def column(block, j):
        at = first + j
        index = jnp.full((TILE, size), at, jnp.int32)
        return tuple(jnp.take_along_axis(b, index, axis=1) for b in block)
    def row(block, j):
        return tuple(jnp.broadcast_to(b[j : j + 1], (TILE, size)) for b in block)
    own = rows[tile]
    columns = [column(own, j) for j in range(TILE)]
    others = [v for v in panel if v != tile]
    if tile + 1 in others:
        others.remove(tile + 1); others.insert(0, tile + 1)
    sides = {v: [column(rows[v], j) for j in range(TILE)] for v in others}
    inside = (lane >= first) & (lane < first + TILE)
    unit = jnp.where(lane - first == sub, 1.0, 0.0)
    own = pick(inside, unit, own)
    for p in range(0, TILE, 2):
        low, high = columns[p], columns[p + 1]
        a, b, d = row(low, p), row(high, p), row(high, p + 1)
        det = minus(times(a, d), times(b, b))
        scale = 1.0 / (det[0] * det[0] + det[1] * det[1])
        q = (det[0] * scale, -det[1] * scale)
        at_low, at_high = sub == p, sub == p + 1
        here = at_low | at_high
        low = pick(at_high, 0.0, pick(at_low, -1.0, low))
        high = pick(at_low, 0.0, pick(at_high, -1.0, high))
        e_low = minus(times(low, d), times(high, b))
        e_high = minus(times(high, a), times(low, b))
        d_low, d_high = times(e_low, q), times(e_high, q)
        for j in range(p + 2, TILE):
            old = columns[j]
            up, down = row(old, p), row(old, p + 1)
            kept = pick(here, 0.0, old)
            change = plus(times(d_low, up), times(d_high, down))
            columns[j] = minus(kept, change)
        up, down = row(own, p), row(own, p + 1)
        own = minus(pick(here, 0.0, own), plus(times(d_low, up), times(d_high, down)))
    rows[tile] = own
    spread = [row(own, j) for j in range(TILE)]
    for v in others:
        change = total([times(sides[v][j], spread[j]) for j in range(TILE)])
        rows[v] = minus(pick(inside, 0.0, rows[v]), change)

def inverse(block, parts=4, ahead=2):
    size = block[0].shape[0]
    lane = lax.broadcasted_iota(jnp.int32, (TILE, size), 1)
    sub = lax.broadcasted_iota(jnp.int32, (TILE, size), 0)
    count = size // TILE
    step = count // parts
    width = step * TILE

    def trip(_, carried):
        rows = [tuple(b[TILE * v : TILE * v + TILE] for b in carried) for v in range(count)]
        ready = list(range(step, step + ahead))
        rest = list(range(step + ahead, count))
        left = jnp.concatenate([carried[0][width + ahead * TILE :], carried[1][width + ahead * TILE :]], axis=1)
        for tile in range(step):
            sweep(rows, tile, list(range(step)) + ready, lane, sub)
        empty = jnp.zeros((size - width, 2 * size), jnp.float32)
        real, imag = (jnp.concatenate([rows[v][c] for v in range(step)], axis=0) for c in (0, 1))
        right = jnp.concatenate(
            [jnp.concatenate([real, imag], axis=1), empty, jnp.concatenate([-imag, real], axis=1), empty], axis=0
        )
        out = dot(left, right)
        gone = lane < width
        for n, v in enumerate(rest):
            part = out[TILE * n : TILE * n + TILE]
            rows[v] = minus(pick(gone, 0.0, rows[v]), (part[:, :size], part[:, size:]))
        order = list(range(step, count)) + list(range(step))
        return tuple(
            pltpu.roll(jnp.concatenate([rows[v][c] for v in order], axis=0), size - width, 1) for c in (0, 1)
        )

    return lax.fori_loop(0, parts // 2, lambda i, c: trip(i, trip(i, c)), block)


def pack(block, row, column):
    diagonal = jnp.sum(jnp.where(row == column, block[1], 0.0), axis=0, keepdims=True)
    return jnp.concatenate(
        [jnp.where(row <= column, block[0], block[1]), jnp.broadcast_to(diagonal, (TILE, block[0].shape[1]))],
        axis=0,
    )


def unpack(packed, row, column):
    size = packed.shape[1]
    block = packed[:size]
    mirror = block.T
    diagonal = packed[size : size + 1]
    return (
        jnp.where(row <= column, block, mirror),
        jnp.where(row == column, diagonal, jnp.where(row > column, block, mirror)),
    )


def wire(count, energy_ref, broad_ref, onsite_ref, mix_ref, hop_ref, hopmix_ref, real_ref, imag_ref,
         crit_out, crit_in, rest_out, rest_in, own_ref, kept_ref, crit_sent, crit_got, rest_sent, rest_got):
    levels = count.bit_length() - 1
    last = levels - 1
    size = mix_ref.shape[1]
    me = lax.axis_index("slab")
    row = lax.broadcasted_iota(jnp.int32, (size, size), 0)
    column = lax.broadcasted_iota(jnp.int32, (size, size), 1)

    def bit(stride):
        return (me // stride) % 2

    def partner(stride):
        return me + stride - 2 * stride * bit(stride)

    def copy(level, stride, out, into, sent, got):
        return pltpu.make_async_remote_copy(
            src_ref=out.at[level], dst_ref=into.at[level], send_sem=sent.at[level],
            recv_sem=got.at[level], device_id={"slab": partner(stride)},
            device_id_type=pl.DeviceIdType.MESH,
        )

    def crit(level, stride):
        return copy(level, stride, crit_out, crit_in, crit_sent, crit_got)

    def rest(level, stride):
        return copy(level, stride, rest_out, rest_in, rest_sent, rest_got)

    def write_rest(level, link, end):
        rest_out[level, :size] = link[0]
        rest_out[level, size : 2 * size] = link[1]
        rest_out[level, 2 * size :] = end

    def link_of(ref, level):
        return (ref[level, :size], ref[level, size : 2 * size])

    barrier = pltpu.get_barrier_semaphore()
    for level in range(levels):
        pl.semaphore_signal(
            barrier, inc=1, device_id={"slab": partner(1 << level)},
            device_id_type=pl.DeviceIdType.MESH,
        )

    unit = row == column
    diagonal_i = jnp.where(unit, broad_ref[0], 0.0)

    def onsite(k):
        mixing = mix_ref[k]
        diagonal = jnp.where(unit, energy_ref[0] - onsite_ref[k : k + 1, :], 0.0)
        return diagonal - 0.5 * (mixing + mixing.T)

    def coupling(k):
        return jnp.where(unit, hop_ref[k : k + 1, :], 0.0) + hopmix_ref[k]

    def halves(out):
        return (out[:, :size], out[:, size:])

    middle = inverse((onsite(1), diagonal_i))
    lower = coupling(0)
    upper = jnp.where(me == count - 1, 0.0, coupling(1))
    lower_t, upper_t = lower.T, upper.T
    high = bit(1) > 0
    both = jnp.concatenate([middle[0], middle[1]], axis=0)
    first = jnp.where(high, lower_t, upper)
    weighted = dot(both, first)
    near = (weighted[:size], weighted[size:])
    outs = halves(dot(jnp.where(high, lower, upper_t), jnp.concatenate(near, axis=1)))
    alpha = pack((onsite(0), diagonal_i), row, column)
    change = pack(outs, row, column)
    crit_out[0] = jnp.where(high, alpha - change, change)
    pl.semaphore_wait(barrier, levels)
    if levels > 1:
        crit(0, 1).start()
    weighted = dot(both, jnp.where(high, upper, lower_t))
    far = (weighted[:size], weighted[size:])
    to_low, to_high = chosen(high, near, far), chosen(high, far, near)
    outs = halves(dot(jnp.where(high, upper_t, lower), jnp.concatenate(far, axis=1)))
    link = halves(dot(lower, jnp.concatenate(to_high, axis=1)))
    change = pack(outs, row, column)
    write_rest(0, link, jnp.where(high, change, alpha - change))
    if levels > 1:
        rest(0, 1).start()
    zero = jnp.zeros((size, size), jnp.float32)
    one = jnp.where(unit, 1.0, 0.0)
    write(own_ref, (zero, zero), 0, 0)
    write(own_ref, (one, zero), 0, 2)
    write(own_ref, (zero, zero), 0, 4)
    write(own_ref, middle, 1, 0)
    write(own_ref, to_low, 1, 2)
    write(own_ref, to_high, 1, 4)

    def eliminated(level, high):
        packed = jnp.where(high, 1.0, -1.0) * (crit_out[level] - crit_in[level])
        return inverse(unpack(packed, row, column))

    def advance(high, y, low_t, high_link):
        legs = cols(low_t, high_link)
        states = [[read(own_ref, k, 2 * piece) for piece in range(3)] for k in range(2)]
        used = [chosen(high, state[1], state[2]) for state in states]
        weighted = product(rows(*used), y)
        moved = product(weighted, legs)
        for k, state in enumerate(states):
            part = slice(k * size, (k + 1) * size)
            own = product((weighted[0][part], weighted[1][part]), flipped(used[k]))
            write(own_ref, tuple(s + o for s, o in zip(state[0], own)), k, 0)
            down = tuple(
                jnp.where(high, 0.0, s) + m[part, :size] for s, m in zip(state[1], moved)
            )
            up = tuple(
                jnp.where(high, s, 0.0) + m[part, size:] for s, m in zip(state[2], moved)
            )
            write(own_ref, down, k, 2)
            write(own_ref, up, k, 4)

    def step(level, stride):
        high = bit(stride) > 0
        crit(level, stride).wait_recv()
        y = eliminated(level, high)
        rest(level, stride).wait_recv()
        mine, other = link_of(rest_out, level), link_of(rest_in, level)
        low_link, high_link = chosen(high, other, mine), chosen(high, mine, other)
        mine, other = rest_out[level, 2 * size :], rest_in[level, 2 * size :]
        alpha, beta = jnp.where(high, other, mine), jnp.where(high, mine, other)
        low_t, high_t = flipped(low_link), flipped(high_link)
        following = bit(2 * stride) > 0
        near = product(chosen(following, low_link, high_t), y)
        change = pack(product(near, chosen(following, low_t, high_link)), row, column)
        crit_out[level + 1] = jnp.where(following, alpha - change, beta + change)

        @pl.when(level + 1 < last)
        def _():
            crit(level + 1, 2 * stride).start()

        far = product(chosen(following, high_t, low_link), y)
        change = pack(product(far, chosen(following, high_link, low_t)), row, column)
        link = product(chosen(following, near, far), high_link)
        write_rest(level + 1, link, jnp.where(following, beta + change, alpha - change))

        kept_ref[0] = y[0]
        kept_ref[1] = y[1]

        @pl.when(level + 1 < last)
        def _():
            rest(level + 1, 2 * stride).start()
            advance(high, y, low_t, high_link)

        return 2 * stride

    stride = lax.fori_loop(0, last, step, jnp.int32(1))
    high = bit(stride) > 0
    mine, end = crit_out[last], rest_out[last, 2 * size :]
    link = link_of(rest_out, last)
    ground = inverse(unpack(jnp.where(high, mine, end), row, column))
    change = pack(product(product(flipped(link), ground), link), row, column)
    crit_out[last] = jnp.where(high, mine, mine + change)
    crit(last, stride).start()
    if last > 0:
        before = bit(stride // 2) > 0
        mine, other = link_of(rest_out, last - 1), link_of(rest_in, last - 1)
        low_link, high_link = chosen(before, other, mine), chosen(before, mine, other)
        advance(before, (kept_ref[0], kept_ref[1]), flipped(low_link), high_link)
    states = [[read(own_ref, k, 2 * piece) for piece in range(3)] for k in range(2)]
    weighted = product(rows(*(state[1] for state in states)), ground)
    moved = product(weighted, link)
    owns, legs = [], []
    for k, state in enumerate(states):
        part = slice(k * size, (k + 1) * size)
        own = product((weighted[0][part], weighted[1][part]), flipped(state[1]))
        owns.append(tuple(s + jnp.where(high, 0.0, o) for s, o in zip(state[0], own)))
        legs.append(
            tuple(jnp.where(high, d, u + m[part]) for d, u, m in zip(state[1], state[2], moved))
        )
    crit(last, stride).wait_recv()
    y = eliminated(last, high)
    weighted = product(rows(*legs), y)
    for k in range(2):
        part = slice(k * size, (k + 1) * size)
        out = product((weighted[0][part], weighted[1][part]), flipped(legs[k]))
        real_ref[k] = owns[k][0] + out[0]
        imag_ref[k] = owns[k][1] + out[1]

    def drain(level, stride):
        crit(level, stride).wait_send()
        rest(level, stride).wait_send()
        return 2 * stride

    stride = lax.fori_loop(0, last, drain, jnp.int32(1))
    crit(last, stride).wait_send()


def shards(onsite_energy, onsite_mixing, hop_strength, hop_mixing, energy, broadening):
    size = onsite_mixing.shape[1]
    count = lax.axis_size("slab")
    levels = count.bit_length() - 1
    vmem = pl.BlockSpec(memory_space=pltpu.VMEM)
    smem = pl.BlockSpec(memory_space=pltpu.SMEM)
    out = jax.ShapeDtypeStruct(onsite_mixing.shape, jnp.float32)
    crit = pltpu.VMEM((levels, size + TILE, size), jnp.float32)
    rest = pltpu.VMEM((levels, 3 * size + TILE, size), jnp.float32)
    return pl.pallas_call(
        functools.partial(wire, count),
        out_shape=[out, out],
        in_specs=[smem] * 2 + [vmem] * 4,
        out_specs=[vmem, vmem],
        scratch_shapes=[crit, crit, rest, rest, pltpu.VMEM((2, 6, size, size), jnp.float32), pltpu.VMEM((2, size, size), jnp.float32)]
        + [pltpu.SemaphoreType.DMA((levels,))] * 4,
        compiler_params=pltpu.CompilerParams(collective_id=0, has_side_effects=True),
        name="wire",
    )(energy, broadening, onsite_energy, onsite_mixing, hop_strength, hop_mixing)


def solution(mesh):
    return jax.shard_map(
        shards,
        mesh=mesh,
        in_specs=(
            P("slab", None),
            P("slab", None, None),
            P("slab", None),
            P("slab", None, None),
            P("energy"),
            P("energy"),
        ),
        out_specs=(P(("energy", "slab"), None, None), P(("energy", "slab"), None, None)),
        check_vma=False,
    )
```
